32 devices in a mesh: batch: 4 (over y, x), mp: 8 (over z, core).
Axes of the slice: x: 2, y: 2, z: 4, core: 2. Of those that a mesh axis runs over, the one named last changes fastest.
Arguments:
- pixels: bfloat16 [8, 8, 4, 100, 768], P('batch', 'mp'), may hold values from -6 to 6
- patch_weight: bfloat16 [768, 1024], P('mp'), may hold values from -0.21875 to 0.21875
- position: bfloat16 [100, 1024], replicated, may hold values from -3 to 3
- encoder_gains: float32 [3, 1024], replicated, may hold values from 0.25 to 1.75
- qkv_weight: bfloat16 [1024, 3072], P('mp'), may hold values from -0.1875 to 0.1875
- out_weight: bfloat16 [1024, 1024], P('mp'), may hold values from -0.1875 to 0.1875
- up_weight: bfloat16 [1024, 4096], P('mp'), may hold values from -0.1875 to 0.1875
- down_weight: bfloat16 [4096, 1024], P('mp'), may hold values from -0.09375 to 0.09375
- cond_weight: bfloat16 [1024, 512], replicated, may hold values from -0.1875 to 0.1875
- time_weight: float32 [512, 512], replicated, may hold values from -0.5 to 0.5
- action_in: float32 [10, 512], replicated, may hold values from -2 to 2
- action_pos: float32 [16, 512], replicated, may hold values from -3 to 3
- denoise_gains: float32 [3, 512], replicated, may hold values from 0.25 to 1.75
- self_qkv: bfloat16 [512, 1536], replicated, may hold values from -0.25 to 0.25
- self_out: bfloat16 [512, 512], replicated, may hold values from -0.25 to 0.25
- cross_query: bfloat16 [512, 512], replicated, may hold values from -0.25 to 0.25
- cross_kv: bfloat16 [512, 1024], replicated, may hold values from -0.25 to 0.25
- cross_out: bfloat16 [512, 512], replicated, may hold values from -0.25 to 0.25
- mix_up: bfloat16 [512, 2048], replicated, may hold values from -0.25 to 0.25
- mix_down: bfloat16 [2048, 512], replicated, may hold values from -0.125 to 0.125
- action_out: float32 [512, 10], replicated, may hold values from -0.25 to 0.25
- noise: float32 [8, 4, 8, 16, 10], P('mp', 'batch'), may hold values from -5 to 5
- timesteps: int32 [4], replicated, may hold values from 5 to 79, as said below
Outputs:
- actions: float32 [8, 4, 8, 16, 10], P('mp', 'batch')
The draws below stay inside these ranges and needn't reach their ends.
Inputs may be any that keep to these rules, and one draw needn't show every extreme that they name: `timesteps`: strictly decreasing.
All inputs are finite; a program needn't handle non-finite values.
Results may differ from the reference program's by a relative error of at most 0.0033.
Values may be sent and summed in bfloat16 or wider, within the bound.
No kernel may reach another device: no remote copies, remote signals or barrier semaphores. Data moves between devices by JAX's collectives and lax.ppermute only.
A program may use at most 192 MiB of HBM per device.

```python
import math
import jax
import jax.numpy as jnp
from jax import lax

D = 1024
HEADS = 16
FF = 4096
GRID = 10
PATCH_PIX = 768
VIEWS = 8
W = 512
DHEADS = 8
DFF = 2048
CAND = 8
SPAN = 16
ACT = 10
STEPS = 4
TMAX = 100
HEAD_DIM = 64
PATCHES = 100
CELLS = 25
DHEAD = 64
GROUPS = 8
BLOCK = 4


def draw_timesteps(key, part):
    order = jax.random.permutation(key, TMAX - 27)
    middle = jnp.sort(order[:STEPS - 2] + 6)[::-1]
    top = jnp.full((1,), TMAX - 21, jnp.int32)
    bottom = jnp.full((1,), 5, jnp.int32)
    return jnp.concatenate([top, middle.astype(jnp.int32), bottom]).astype(jnp.int32)


def block_levels(own_key, dims, shards, least, top_value):
    level, own = 1.0, jax.random.fold_in(own_key, 6)
    for dim, blocks in shards:
        steps = jnp.exp(jax.random.uniform(jax.random.fold_in(own, dim), (blocks,), jnp.float32, least / len(shards), top_value / len(shards)))
        level = level * jnp.repeat(steps, dims[dim] // blocks).reshape([-1 if axis == dim else 1 for axis in range(len(dims))])
    return level


def normal_values(stream_key, shape, scale, most, shards=(), held_as=jnp.bfloat16):
    entries = jax.random.normal(stream_key, shape, jnp.float32) * scale
    if len(shards) > 0:
        entries = block_levels(stream_key, shape, shards, -0.22, 0.18) * entries
    return jnp.clip(entries, min=-most, max=most).astype(held_as)


def setup_inputs(seed: int = 0) -> dict:
    streams_of = jax.random.split(jax.random.key(seed), 24)
    pixels = normal_values(streams_of[0], (VIEWS, GROUPS, BLOCK, PATCHES, PATCH_PIX), 1.0, 6.0, ((0, 4), (1, 8)))
    patch_weight = normal_values(streams_of[1], (PATCH_PIX, D), PATCH_PIX ** -0.5, 0.21875, ((0, 8),))
    position = normal_values(streams_of[2], (PATCHES, D), 0.5, 3.0)
    encoder_gains = jnp.clip(1.0 + 0.15 * jax.random.normal(streams_of[3], (3, D), jnp.float32), 0.25, 1.75)
    qkv_weight = normal_values(streams_of[4], (D, 3 * D), D ** -0.5, 0.1875, ((0, 8),))
    out_weight = normal_values(streams_of[5], (D, D), D ** -0.5, 0.1875, ((0, 8),))
    up_weight = normal_values(streams_of[6], (D, FF), D ** -0.5, 0.1875, ((0, 8),))
    down_weight = normal_values(streams_of[7], (FF, D), FF ** -0.5, 0.09375, ((0, 8),))
    cond_weight = normal_values(streams_of[8], (D, W), D ** -0.5, 0.1875)
    time_weight = normal_values(streams_of[9], (W, W), (W // 4) ** -0.5, 0.5, (), jnp.float32)
    action_in = normal_values(streams_of[10], (ACT, W), ACT ** -0.5, 2.0, (), jnp.float32)
    action_pos = normal_values(streams_of[11], (SPAN, W), 0.5, 3.0, (), jnp.float32)
    denoise_gains = jnp.clip(1.0 + 0.15 * jax.random.normal(streams_of[12], (3, W), jnp.float32), 0.25, 1.75)
    self_qkv = normal_values(streams_of[13], (W, 3 * W), W ** -0.5, 0.25)
    self_out = normal_values(streams_of[14], (W, W), W ** -0.5, 0.25)
    cross_query = normal_values(streams_of[15], (W, W), W ** -0.5, 0.25)
    cross_kv = normal_values(streams_of[16], (W, 2 * W), W ** -0.5, 0.25)
    cross_out = normal_values(streams_of[17], (W, W), W ** -0.5, 0.25)
    mix_up = normal_values(streams_of[18], (W, DFF), W ** -0.5, 0.25)
    mix_down = normal_values(streams_of[19], (DFF, W), DFF ** -0.5, 0.125)
    action_out = normal_values(streams_of[20], (W, ACT), W ** -0.5, 0.25, (), jnp.float32)
    noise = normal_values(streams_of[21], (GROUPS, BLOCK, CAND, SPAN, ACT), 1.0, 5.0, ((0, 8), (1, 4)), jnp.float32)
    timesteps = draw_timesteps(jax.random.fold_in(streams_of[23], 71), 0)
    return {"pixels": pixels, "patch_weight": patch_weight, "position": position, "encoder_gains": encoder_gains, "qkv_weight": qkv_weight, "out_weight": out_weight, "up_weight": up_weight, "down_weight": down_weight, "cond_weight": cond_weight, "time_weight": time_weight, "action_in": action_in, "action_pos": action_pos, "denoise_gains": denoise_gains, "self_qkv": self_qkv, "self_out": self_out, "cross_query": cross_query, "cross_kv": cross_kv, "cross_out": cross_out, "mix_up": mix_up, "mix_down": mix_down, "action_out": action_out, "noise": noise, "timesteps": timesteps}


norm_eps = 1e-06
offset = 0.008

def normalize(values, gain):
    middle = lax.optimization_barrier(jnp.mean(values, -1, keepdims=True))
    centred = values - middle
    spread = lax.optimization_barrier(jnp.mean(centred * centred, -1, keepdims=True))
    return centred * lax.rsqrt(spread + norm_eps) * gain

def plan(level):
    angle = (level.astype(jnp.float32) / TMAX + offset) / (1.0 + offset) * (math.pi / 2)
    base = math.cos(offset / (1.0 + offset) * math.pi / 2) ** 2
    return jnp.cos(angle) ** 2 / base

def product(left, right):
    return jnp.dot(left, right, preferred_element_type=jnp.float32)

def precise(left, right):
    return jnp.dot(left, right, precision=lax.Precision.HIGHEST)

def encode(frames, patch_weight, position, encoder_gains, qkv_weight, out_weight, up_weight, down_weight):
    count = frames.shape[0]
    state = product(frames.reshape(-1, PATCH_PIX), patch_weight).reshape(count, PATCHES, D)
    state = state + position.astype(jnp.float32)
    normed = normalize(state, encoder_gains[0]).astype(jnp.bfloat16).reshape(-1, D)
    packed = product(normed, qkv_weight).astype(jnp.bfloat16).reshape(count, PATCHES, 3, HEADS, HEAD_DIM)
    query = packed[:, :, 0].astype(jnp.float32)
    keys = packed[:, :, 1].astype(jnp.float32)
    values = packed[:, :, 2].astype(jnp.float32)
    scores = jnp.einsum('nqhd,nkhd->nhqk', query, keys) / math.sqrt(HEAD_DIM)
    probs = jax.nn.softmax(scores, -1).astype(jnp.bfloat16)
    context = jnp.einsum('nhqk,nkhd->nqhd', probs.astype(jnp.float32), values).astype(jnp.bfloat16)
    state = state + product(context.reshape(-1, D), out_weight).reshape(count, PATCHES, D)
    normed = normalize(state, encoder_gains[1]).astype(jnp.bfloat16).reshape(-1, D)
    hidden = jax.nn.gelu(product(normed, up_weight), approximate=False).astype(jnp.bfloat16)
    state = state + product(hidden, down_weight).reshape(count, PATCHES, D)
    final = normalize(state, encoder_gains[2]).reshape(count, GRID // 2, 2, GRID // 2, 2, D)
    return lax.optimization_barrier(jnp.mean(final, axis=(2, 4))).reshape(count, CELLS, D).astype(jnp.bfloat16)

def predict(sample, level, memory, params):
    time_weight, action_in, action_pos, gains, self_qkv, self_out, cross_query, cross_out, mix_up, mix_down, action_out = params
    samples = sample.shape[0]
    half = W // 2
    freqs = jnp.exp(-math.log(10000.0) * jnp.arange(half, dtype=jnp.float32) / half)
    phase = level.astype(jnp.float32) * freqs
    stamp = precise(jnp.concatenate([jnp.sin(phase), jnp.cos(phase)])[None, :], time_weight)[0]
    state = precise(sample.reshape(-1, ACT), action_in).reshape(samples, CAND, SPAN, W) + action_pos + stamp
    normed = normalize(state, gains[0]).astype(jnp.bfloat16).reshape(-1, W)
    packed = product(normed, self_qkv).astype(jnp.bfloat16).reshape(samples, CAND, SPAN, 3, DHEADS, DHEAD)
    query = packed[:, :, :, 0].astype(jnp.float32)
    keys = packed[:, :, :, 1].astype(jnp.float32)
    values = packed[:, :, :, 2].astype(jnp.float32)
    scores = jnp.einsum('sctgd,scugd->scgtu', query, keys) / math.sqrt(DHEAD)
    probs = jax.nn.softmax(scores, -1).astype(jnp.bfloat16)
    context = jnp.einsum('scgtu,scugd->sctgd', probs.astype(jnp.float32), values).astype(jnp.bfloat16)
    state = state + product(context.reshape(-1, W), self_out).reshape(state.shape)
    normed = normalize(state, gains[1]).astype(jnp.bfloat16).reshape(-1, W)
    asked = product(normed, cross_query).astype(jnp.bfloat16).reshape(samples, CAND * SPAN, DHEADS, DHEAD)
    length = memory.shape[1]
    far_keys = memory[:, :, :W].reshape(samples, length, DHEADS, DHEAD).astype(jnp.float32)
    far_values = memory[:, :, W:].reshape(samples, length, DHEADS, DHEAD).astype(jnp.float32)
    scores = jnp.einsum('sqgd,skgd->sgqk', asked.astype(jnp.float32), far_keys) / math.sqrt(DHEAD)
    probs = jax.nn.softmax(scores, -1).astype(jnp.bfloat16)
    context = jnp.einsum('sgqk,skgd->sqgd', probs.astype(jnp.float32), far_values).astype(jnp.bfloat16)
    state = state + product(context.reshape(-1, W), cross_out).reshape(state.shape)
    normed = normalize(state, gains[2]).astype(jnp.bfloat16).reshape(-1, W)
    hidden = jax.nn.gelu(product(normed, mix_up), approximate=False).astype(jnp.bfloat16)
    state = state + product(hidden, mix_down).reshape(state.shape)
    return precise(state.reshape(-1, W), action_out).reshape(sample.shape)

def reference(pixels, patch_weight, position, encoder_gains, qkv_weight, out_weight, up_weight, down_weight, cond_weight, time_weight, action_in, action_pos, denoise_gains, self_qkv, self_out, cross_query, cross_kv, cross_out, mix_up, mix_down, action_out, noise, timesteps):
    blocks = pixels.reshape(VIEWS * GROUPS, BLOCK, PATCHES, PATCH_PIX)

    def encode_block(frames):
        return encode(frames, patch_weight, position, encoder_gains, qkv_weight, out_weight, up_weight, down_weight)
    pooled = lax.map(encode_block, blocks)
    condition = product(pooled.reshape(-1, D), cond_weight).astype(jnp.bfloat16)
    memory = product(condition, cross_kv).astype(jnp.bfloat16)
    memory = memory.reshape(VIEWS, GROUPS, BLOCK, CELLS, 2 * W)
    memory = jnp.transpose(memory, (1, 2, 0, 3, 4)).reshape(GROUPS * BLOCK, VIEWS * CELLS, 2 * W)
    params = (time_weight, action_in, action_pos, denoise_gains, self_qkv, self_out, cross_query, cross_out, mix_up, mix_down, action_out)
    sample = noise.reshape(GROUPS * BLOCK, CAND, SPAN, ACT)
    for step in range(STEPS):
        level = timesteps[step]
        current = plan(level)
        if step + 1 < STEPS:
            after = plan(timesteps[step + 1])
        else:
            after = jnp.ones((), jnp.float32)
        predicted = predict(sample, level, memory, params)
        clean = (sample - jnp.sqrt(1.0 - current) * predicted) / jnp.sqrt(current)
        sample = jnp.sqrt(after) * clean + jnp.sqrt(1.0 - after) * predicted
    return sample.reshape(noise.shape)
```

```python
import functools
import math

import jax
import jax.numpy as jnp
from jax import lax
from jax.experimental import pallas as pl
from jax.experimental.pallas import tpu as pltpu
from jax.sharding import PartitionSpec as P

HEADS = 16
GRID = 10
DHEADS = 8
STEPS = 4
TMAX = 100

norm_eps = 1e-06
offset = 0.008
LANES = 128
NEG = -1e30


def up_to(value, step):
    return -(-value // step) * step


def normalize(values, gain):
    middle = jnp.mean(values, -1, keepdims=True)
    centred = values - middle
    spread = jnp.mean(centred * centred, -1, keepdims=True)
    return centred * lax.rsqrt(spread + norm_eps) * gain


def gelu(values):
    return 0.5 * values * (1.0 + lax.erf(values * math.sqrt(0.5)))


def plan(level):
    angle = (level.astype(jnp.float32) / TMAX + offset) / (1.0 + offset) * (math.pi / 2)
    base = math.cos(offset / (1.0 + offset) * math.pi / 2) ** 2
    return jnp.cos(angle) ** 2 / base


def product(left, right):
    return jnp.dot(left, right, preferred_element_type=jnp.float32)


def product_t(left, right):
    return lax.dot_general(
        left, right, (((1,), (1,)), ((), ())), preferred_element_type=jnp.float32
    )


def precise(left, right):
    return jnp.dot(
        left, right, precision=lax.Precision.HIGHEST, preferred_element_type=jnp.float32
    )


def assemble(places, index, layout, pieces):
    spot, shard = index[0], index[1]
    z, core = shard // 2, shard % 2
    members = len(places)
    own, partner, rest = pieces[:members], pieces[members : 2 * members], pieces[2 * members :]
    sides = ((core, rest[:5]), (1 - core, rest[5:]))
    length = sum(rows * groups for _, rows, groups in layout)
    total, width = rest[0].shape
    depth = total // length
    half = rest[3].shape[0]
    for place, mine, theirs, (first, rows, groups) in zip(places, own, partner, layout):
        wide = place.shape[1] // groups
        place[pl.ds(pl.multiple_of(shard * rows, 16), rows), :] = mine[...]
        place[pl.ds(pl.multiple_of((z * 2 + 1 - core) * rows, 16), rows), :] = theirs[...]
        for turn in range(depth):
            other = lax.rem(z + 2 * (depth + 1) - turn - 1, depth + 1)
            for side, parts in sides:
                row = (other * 2 + side) * rows
                for quarter in range(4):
                    column = (spot ^ quarter) * width
                    for group in range(groups):
                        start = turn * length + first + group * rows
                        at = pl.multiple_of(group * wide + column, width)
                        if quarter < 3:
                            spans = [(parts[quarter], start, 0, rows)]
                        else:
                            top = min(max(half - start, 0), rows)
                            spans = [(parts[3], start, 0, top), (parts[4], start + top - half, top, rows)]
                        for source, begin, low, high in spans:
                            if high > low:
                                place[
                                    pl.ds(pl.multiple_of(row + low, 16), high - low),
                                    pl.ds(at, width),
                                ] = source[begin : begin + high - low, :]


def load(places, index, layout, pieces):
    if layout is None:
        return pieces
    assemble(places, index, layout, pieces)
    return places


def by_tiles(wide, step, body):
    def one(tile, carry):
        body(pl.ds(pl.multiple_of(tile * step, step), step))
        return carry

    lax.fori_loop(0, wide // step, one, 0)


def by_frames(count, full, body):
    def one(frame, carry):
        body(frame, pl.ds(pl.multiple_of(frame * full, 16), full))
        return carry

    lax.fori_loop(0, count, one, 0)


def quarter_kernel(layouts, index, *refs):
    weights, outs = refs[: -len(layouts)], refs[-len(layouts) :]
    at = 0
    for layout, out in zip(layouts, outs):
        width = out.shape[1]
        for first, rows, groups in layout:
            weight = weights[at]
            at += 1
            wide = weight.shape[1] // groups
            for group in range(groups):
                column = pl.multiple_of(group * wide + index[0] * width, width)
                start = first + group * rows
                out[start : start + rows, :] = weight[:, pl.ds(column, width)]


def pack_kernel(*refs):
    out, start = refs[-1], 0
    for ref in refs[:-1]:
        out[start : start + ref.shape[0], :] = ref[...]
        start += ref.shape[0]


def embed_kernel(layout, patches, index, pixels, position, gains, *refs):
    pieces, (state, packed, place, more, rows, offset_rows, normed) = refs[:-7], refs[-7:]
    weight, qkv = load((place, more), index, layout, pieces)
    count = pixels.shape[0]
    full = rows.shape[0] // count
    rows[...] = jnp.zeros(rows.shape, rows.dtype)
    offset_rows[...] = jnp.zeros(offset_rows.shape, jnp.float32)
    offset_rows[:patches, :] = position[...].astype(jnp.float32)
    for frame in range(count):
        rows[frame * full : frame * full + patches, :] = pixels[frame]

    def fill(tile):
        value = product(rows[...], weight[:, tile])
        state[:, tile] = (
            value.reshape(count, full, value.shape[1]) + offset_rows[:, tile][None]
        ).reshape(value.shape)

    by_tiles(state.shape[1], 256, fill)

    def settle(frame, at):
        normed[at, :] = normalize(state[at, :], gains[0:1, :]).astype(jnp.bfloat16)

    by_frames(count, full, settle)

    def spread(tile):
        packed[:, tile] = product(normed[...], qkv[:, tile]).astype(jnp.bfloat16)

    by_tiles(packed.shape[1], 512, spread)


def pair_sums(length, head):
    row = lax.broadcasted_iota(jnp.int32, (2 * length, LANES), 0)
    lane = lax.broadcasted_iota(jnp.int32, (2 * length, LANES), 1)
    return jnp.where((row < length) == (lane < head), 1.0, 0.0).astype(jnp.bfloat16)


def weigh(scores, valid, values):
    size = scores.shape[1] // 2
    done = []
    for part in range(2):
        own = jnp.where(valid, scores[:, part * size : (part + 1) * size], NEG)
        done.append(jnp.exp(own - jnp.max(own, -1, keepdims=True)).astype(jnp.bfloat16))
    both = product(jnp.concatenate(done, 1), values)
    return (both[:, :LANES] / both[:, LANES:]).astype(jnp.bfloat16)


def attend_kernel(patches, packed, context, keys, values):
    rows, width = context.shape
    full = up_to(patches, 16)
    count = rows // full
    head = width // HEADS
    scale = 1.0 / math.sqrt(head)
    lane = lax.broadcasted_iota(jnp.int32, (full, LANES), 1)
    first = lane < head
    valid = lane < patches
    pairs = width // LANES
    sums = pair_sums(LANES, head)
    for pair in range(pairs):
        keys[pair] = jnp.zeros((2 * LANES, LANES), jnp.bfloat16)
        values[pair, :, :LANES] = jnp.zeros((2 * LANES, LANES), jnp.bfloat16)
        values[pair, :, LANES:] = sums
    zero = jnp.zeros((full, LANES), jnp.bfloat16)

    def one(frame, at):
        for pair in range(pairs):
            left = pair * LANES
            query = packed[at, left : left + LANES]
            key = packed[at, width + left : width + left + LANES]
            value = packed[at, 2 * width + left : 2 * width + left + LANES]
            keys[pair, 0:full, :] = jnp.where(first, key, zero)
            keys[pair, LANES : LANES + full, :] = jnp.where(first, zero, key)
            values[pair, 0:full, :LANES] = jnp.where(first, value, zero)
            values[pair, LANES : LANES + full, :LANES] = jnp.where(first, zero, value)
            scores = product_t(query, keys[pair]) * scale
            context[at, left : left + LANES] = weigh(scores, valid, values[pair])

    by_frames(count, full, one)


def mix_kernel(layout, patches, index, state, context, gains, *refs):
    pieces, (after, hidden, out_place, up_place, normed) = refs[:-5], refs[-5:]
    out_weight, up_weight = load((out_place, up_place), index, layout, pieces)
    rows, width = state.shape
    full = up_to(patches, 16)

    def turn(tile):
        after[:, tile] = state[:, tile] + product(context[...], out_weight[:, tile])

    by_tiles(width, 256, turn)

    def settle(frame, at):
        normed[at, :] = normalize(after[at, :], gains[1:2, :]).astype(jnp.bfloat16)

    by_frames(rows // full, full, settle)

    def fill(tile):
        hidden[:, tile] = gelu(product(normed[...], up_weight[:, tile])).astype(jnp.bfloat16)

    by_tiles(hidden.shape[1], 256, fill)


def pool_kernel(layout, patches, index, state, hidden, gains, cond_weight, *refs):
    pieces, (condition, place, after, pooled) = refs[:-4], refs[-4:]
    (weight,) = load((place,), index, layout, pieces)
    rows, width = state.shape
    full = up_to(patches, 16)
    count = rows // full
    side = GRID // 2
    cells = pooled.shape[0] // count

    def turn(tile):
        after[:, tile] = state[:, tile] + product(hidden[...], weight[:, tile])

    by_tiles(width, 256, turn)
    cell = lax.broadcasted_iota(jnp.int32, (cells, full), 0)
    patch = lax.broadcasted_iota(jnp.int32, (cells, full), 1)
    target = (patch // GRID) // 2 * side + (patch % GRID) // 2
    mean = jnp.where((target == cell) & (patch < patches), 0.25, 0.0).astype(jnp.float32)

    def settle(frame, at):
        value = normalize(after[at, :], gains[2:3, :])
        start = pl.multiple_of(frame * cells, 16)
        pooled[pl.ds(start, cells), :] = precise(mean, value).astype(jnp.bfloat16)

    by_frames(count, full, settle)
    condition[...] = product(pooled[...], cond_weight[...]).astype(jnp.bfloat16)


def denoise_kernel(
    cells,
    terms,
    condition,
    sample_in,
    base,
    action_in,
    gains,
    self_qkv,
    self_out,
    cross_query,
    cross_kv,
    cross_out,
    mix_up,
    mix_down,
    action_out,
    result,
    far_keys,
    far_values,
):
    tokens = sample_in.shape[0]
    width = self_out.shape[0]
    span = base.shape[1]
    head = width // DHEADS
    scale = 1.0 / math.sqrt(head)
    pairs = width // LANES
    length = condition.shape[0]
    padded = cells[1]
    memory = product(condition[...], cross_kv[...]).astype(jnp.bfloat16)
    first = lax.broadcasted_iota(jnp.int32, (length, LANES), 1) < head
    zero = jnp.zeros((length, LANES), jnp.bfloat16)
    far_sums = pair_sums(length, head)
    near_sums = pair_sums(tokens, head)
    for pair in range(pairs):
        left = pair * LANES
        key = memory[:, left : left + LANES]
        value = memory[:, width + left : width + left + LANES]
        far_keys[pair, :length, :] = jnp.where(first, key, zero)
        far_keys[pair, length:, :] = jnp.where(first, zero, key)
        far_values[pair, :length, :LANES] = jnp.where(first, value, zero)
        far_values[pair, length:, :LANES] = jnp.where(first, zero, value)
        far_values[pair, :, LANES:] = far_sums
    seen = lax.broadcasted_iota(jnp.int32, (tokens, length), 1) % padded < cells[0]
    row = lax.broadcasted_iota(jnp.int32, (tokens, tokens), 0)
    column = lax.broadcasted_iota(jnp.int32, (tokens, tokens), 1)
    same = row // span == column // span
    near = lax.broadcasted_iota(jnp.int32, (tokens, LANES), 1) < head
    none = jnp.zeros((tokens, LANES), jnp.bfloat16)
    sample = sample_in[...]
    for step in range(STEPS):
        state = precise(sample, action_in[...])
        place = base[step]
        state = (state.reshape(tokens // span, span, width) + place[None]).reshape(tokens, width)
        normed = normalize(state, gains[0:1, :]).astype(jnp.bfloat16)
        packed = product(normed, self_qkv[...]).astype(jnp.bfloat16)
        heads = []
        for pair in range(pairs):
            left = pair * LANES
            query = packed[:, left : left + LANES]
            key = packed[:, width + left : width + left + LANES]
            value = packed[:, 2 * width + left : 2 * width + left + LANES]
            both = jnp.concatenate([jnp.where(near, key, none), jnp.where(near, none, key)], 0)
            scores = product_t(query, both) * scale
            both = jnp.concatenate([jnp.where(near, value, none), jnp.where(near, none, value)], 0)
            heads.append(weigh(scores, same, jnp.concatenate([both, near_sums], 1)))
        state = state + product(jnp.concatenate(heads, 1), self_out[...])
        normed = normalize(state, gains[1:2, :]).astype(jnp.bfloat16)
        asked = product(normed, cross_query[...]).astype(jnp.bfloat16)
        heads = []
        for pair in range(pairs):
            left = pair * LANES
            scores = product_t(asked[:, left : left + LANES], far_keys[pair]) * scale
            heads.append(weigh(scores, seen, far_values[pair]))
        state = state + product(jnp.concatenate(heads, 1), cross_out[...])
        normed = normalize(state, gains[2:3, :]).astype(jnp.bfloat16)
        hidden = gelu(product(normed, mix_up[...])).astype(jnp.bfloat16)
        state = state + product(hidden, mix_down[...])
        predicted = precise(state, action_out[...])
        clean = (sample - terms[step, 0] * predicted) / terms[step, 1]
        sample = terms[step, 2] * clean + terms[step, 3] * predicted
    result[...] = sample


def call(name, kernel, outs, scratch, smem, flops, *args):
    space = pl.BlockSpec(memory_space=pltpu.VMEM)
    with jax.named_scope(name):
        return pl.pallas_call(
            kernel,
            out_shape=outs,
            in_specs=[pl.BlockSpec(memory_space=pltpu.SMEM)] * smem
            + [space] * (len(args) - smem),
            out_specs=jax.tree.map(lambda _: space, outs),
            scratch_shapes=scratch,
            cost_estimate=pl.CostEstimate(flops=flops, transcendentals=0, bytes_accessed=0),
            compiler_params=pltpu.CompilerParams(vmem_limit_bytes=58 * 1024 * 1024),
        )(*args)


def send(name, value, axis, pairs):
    with jax.named_scope(name):
        return lax.ppermute(value, axis, pairs)


def collect(chunks, quarters, planes):
    turns = [
        [(core + 2 * z, core + 2 * ((z + turn) % planes)) for z in range(planes) for core in (0, 1)]
        for turn in range(1, planes)
    ]
    across = [(i, i ^ 1) for i in range(4)]
    along = [(i, i ^ 2) for i in range(4)]
    trade = [(i, i ^ 1) for i in range(2 * planes)]
    done = []
    for k, (weights, quarter) in enumerate(zip(chunks, quarters)):
        partner = [send(f"own{k}_{j}", w, "mp", trade) for j, w in enumerate(weights)]
        parts = [send(f"z{k}_{j}", quarter, "mp", turn) for j, turn in enumerate(turns)]
        rows, width = quarter.shape
        far = call(
            f"pack{k}",
            pack_kernel,
            jax.ShapeDtypeStruct((rows * len(parts), width), quarter.dtype),
            [],
            0,
            10**6,
            *parts,
        )
        right = send(f"x{k}", far, "batch", across)
        below = send(f"y{k}", far, "batch", along)
        half = up_to(far.shape[0] // 2, 16)
        top = send(f"dx{k}", below[:half], "batch", across)
        low = send(f"dy{k}", right[half:], "batch", along)
        mine = [far, right, below, top, low]
        theirs = [send(f"s{k}_{j}", piece, "mp", trade) for j, piece in enumerate(mine)]
        done.append((*weights, *partner, *mine, *theirs))
    return done


def on_device(
    ranks,
    pixels,
    patch_weight,
    position,
    encoder_gains,
    qkv_weight,
    out_weight,
    up_weight,
    down_weight,
    cond_weight,
    time_weight,
    action_in,
    action_pos,
    denoise_gains,
    self_qkv,
    self_out,
    cross_query,
    cross_kv,
    cross_out,
    mix_up,
    mix_down,
    action_out,
    noise,
    timesteps,
):
    local_views, group_count, block_count, patches, pixel_width = pixels.shape
    count = local_views * group_count * block_count
    width = position.shape[1]
    full = up_to(patches, 16)
    batch, shards = ranks
    index = jnp.stack([lax.axis_index("batch"), lax.axis_index("mp")]).astype(jnp.int32)
    weights = (patch_weight, qkv_weight, out_weight, up_weight, down_weight)
    tall = [w.shape[0] * shards for w in weights]
    split = batch == 4 and shards % 2 == 0 and shards > 2 and width % (4 * LANES) == 0
    f32, bf16 = jnp.float32, jnp.bfloat16
    shape = jax.ShapeDtypeStruct
    members = ((0, 1), (2, 3), (4,))
    if split:
        layouts = []
        for chunk in members:
            first, layout = 0, []
            for member in chunk:
                rows, wide = weights[member].shape
                layout.append((first, rows, wide // width))
                first += rows * (wide // width)
            layouts.append(layout)
        quarters = call(
            "quarter",
            functools.partial(quarter_kernel, layouts),
            tuple(
                shape((sum(rows * groups for _, rows, groups in layout), width // 4), bf16)
                for layout in layouts
            ),
            [],
            1,
            10**6,
            index,
            *weights,
        )
        chunks = [[weights[member] for member in chunk] for chunk in members]
        pieces = collect(chunks, quarters, shards // 2)
    else:
        whole = [lax.all_gather(w, "mp", axis=0, tiled=True) for w in weights]
        pieces = [tuple(whole[member] for member in chunk) for chunk in members]
        layouts = [None] * len(members)

    def place(member):
        if split:
            return pltpu.VMEM((tall[member], weights[member].shape[1]), bf16)
        return pltpu.VMEM((16, LANES), bf16)

    def ops(*wanted):
        return 2 * count * full * sum(tall[m] * weights[m].shape[1] for m in wanted)

    rows = count * full
    state, packed = call(
        "embed",
        functools.partial(embed_kernel, layouts[0], patches),
        (shape((rows, width), f32), shape((rows, qkv_weight.shape[1]), bf16)),
        [
            place(0),
            place(1),
            pltpu.VMEM((rows, pixel_width), bf16),
            pltpu.VMEM((full, width), f32),
            pltpu.VMEM((rows, width), bf16),
        ],
        1,
        ops(0, 1),
        index,
        pixels.reshape(count, patches, pixel_width),
        position,
        encoder_gains,
        *pieces[0],
    )
    context = call(
        "attend",
        functools.partial(attend_kernel, patches),
        shape((rows, width), bf16),
        [
            pltpu.VMEM((width // LANES, 2 * LANES, LANES), bf16),
            pltpu.VMEM((width // LANES, 2 * LANES, 2 * LANES), bf16),
        ],
        0,
        ops(1) * 2,
        packed,
    )
    state, hidden = call(
        "mix",
        functools.partial(mix_kernel, layouts[1], patches),
        (shape((rows, width), f32), shape((rows, up_weight.shape[1]), bf16)),
        [place(2), place(3), pltpu.VMEM((rows, width), bf16)],
        1,
        ops(2, 3) * 2,
        index,
        state,
        context,
        encoder_gains,
        *pieces[1],
    )
    cells = (GRID // 2) ** 2
    padded = up_to(cells, 16)
    small = cond_weight.shape[1]
    condition = call(
        "pool",
        functools.partial(pool_kernel, layouts[2], patches),
        shape((count * padded, small), bf16),
        [place(4), pltpu.VMEM((rows, width), f32), pltpu.VMEM((count * padded, width), bf16)],
        1,
        ops(4),
        index,
        state,
        hidden,
        encoder_gains,
        cond_weight,
        *pieces[2],
    )
    condition = condition.reshape(local_views, group_count, block_count, padded, small)
    moved = lax.all_to_all(condition, "batch", split_axis=2, concat_axis=0, tiled=True)
    half = small // 2
    freqs = jnp.exp(-math.log(10000.0) * jnp.arange(half, dtype=f32) / half)
    phase = timesteps.astype(f32)[:, None] * freqs
    stamp = precise(jnp.concatenate([jnp.sin(phase), jnp.cos(phase)], 1), time_weight)
    base = action_pos[None] + stamp[:, None]
    current = plan(timesteps)
    after = jnp.concatenate([current[1:], jnp.ones((1,), f32)])
    terms = jnp.stack(
        [jnp.sqrt(1.0 - current), jnp.sqrt(current), jnp.sqrt(after), jnp.sqrt(1.0 - after)], 1
    )
    cands, span, action_size = noise.shape[2:]
    tokens = cands * span
    extra = up_to(action_size, LANES) - action_size
    observations = noise.shape[0] * noise.shape[1]
    results = []
    for observation in range(observations):
        row, col = divmod(observation, noise.shape[1])
        results.append(
            call(
                "denoise",
                functools.partial(denoise_kernel, (cells, padded)),
                shape((tokens, action_size + extra), f32),
                [
                    pltpu.VMEM((small // LANES, 2 * moved.shape[0] * padded, LANES), bf16),
                    pltpu.VMEM((small // LANES, 2 * moved.shape[0] * padded, 2 * LANES), bf16),
                ],
                1,
                10**10,
                terms,
                moved[:, row, col].reshape(-1, small),
                jnp.pad(noise[row, col].reshape(tokens, action_size), ((0, 0), (0, extra))),
                base,
                jnp.pad(action_in, ((0, extra), (0, 0))),
                denoise_gains,
                self_qkv,
                self_out,
                cross_query,
                cross_kv,
                cross_out,
                mix_up,
                mix_down,
                jnp.pad(action_out, ((0, 0), (0, extra))),
            )[:, :action_size]
        )
    return jnp.stack(results).reshape(noise.shape)


def solution(mesh):
    ranks = (mesh.shape["batch"], mesh.shape["mp"])
    return jax.shard_map(
        functools.partial(on_device, ranks),
        mesh=mesh,
        in_specs=(
            P("batch", "mp", None, None, None),
            P("mp", None),
            P(),
            P(),
            P("mp", None),
            P("mp", None),
            P("mp", None),
            P("mp", None),
            P(),
            P(),
            P(),
            P(),
            P(),
            P(),
            P(),
            P(),
            P(),
            P(),
            P(),
            P(),
            P(),
            P("mp", "batch", None, None, None),
            P(),
        ),
        out_specs=P("mp", "batch", None, None, None),
        check_vma=False,
    )
```
